32 devices in a mesh: seq: 16 (over z, y, x), head: 2 (over core).
Axes of the slice: x: 2, y: 2, z: 4, core: 2. Of those that a mesh axis runs over, the one named last changes fastest.
Arguments:
- queries: bfloat16 [4096, 3584], P('seq', 'head'), may hold values from -5 to 5
- keys: bfloat16 [4096, 3584], P('seq', 'head'), may hold values from -5 to 5
- values: bfloat16 [4096, 3584], P('seq', 'head'), may hold values from -6 to 6
- attn_grad: bfloat16 [4096, 3584], P('seq', 'head'), may hold values from -6 to 6
- doc_ids: int32 [4096], replicated, may hold values from 0 to 3, never falling along the last dimension, each value on 1 to 2048 neighbouring positions
- conv_input: bfloat16 [4096, 7168], P('seq', 'head'), may hold values from -6 to 6
- conv_weight: float32 [4, 7168], P(None, 'head'), may hold values from -3 to 3
- step_raw: float32 [4096, 112], P('seq', 'head'), may hold values from -4 to 4
- step_bias: float32 [112], P('head'), may hold values from -1.5 to 0
- rate_log: float32 [112], P('head'), may hold values from -13 to -1
- skip_gain: float32 [112], P('head'), may hold values from 0.5 to 1.5
- input_coeff: bfloat16 [4096, 128], P('seq'), may hold values from -0.625 to 0.625
- output_coeff: bfloat16 [4096, 128], P('seq'), may hold values from -0.625 to 0.625
- gate_input: bfloat16 [4096, 7168], P('seq', 'head'), may hold values from -6 to 6
- mix_grad: bfloat16 [4096, 7168], P('seq', 'head'), may hold values from -1.5 to 1.5
Outputs:
- grad_queries: bfloat16 [4096, 3584], P('seq', 'head')
- grad_keys: bfloat16 [4096, 3584], P('seq', 'head')
- grad_values: bfloat16 [4096, 3584], P('seq', 'head')
- grad_conv_input: bfloat16 [4096, 7168], P('seq', 'head')
- grad_gate: bfloat16 [4096, 7168], P('seq', 'head')
- grad_step: float32 [4096, 112], P('seq', 'head')
- grad_input_coeff: float32 [4096, 128], P('seq')
- grad_output_coeff: float32 [4096, 128], P('seq')
- grad_conv_weight: float32 [4, 7168], P(None, 'head')
- grad_step_bias: float32 [112], P('head')
- grad_rate_log: float32 [112], P('head')
- grad_skip: float32 [112], P('head')
The draws below stay inside these ranges and needn't reach their ends.
Inputs may be any that keep to these rules, and one draw needn't show every extreme that they name: doc_ids never fall along the sequence.
All inputs are finite; a program needn't handle non-finite values.
Results may differ from the reference program's by a relative error of at most 0.012.
Values may be sent and summed in bfloat16 or wider, within the bound.
A program may use at most 192 MiB of HBM per device.

```python
import math
import jax
import jax.numpy as jnp
import numpy as np
from jax import lax

T_DEV = 256
HEADS = 16
HEAD_DIM = 224
WINDOW = 1024
SSM_HEADS = 112
SSM_DIM = 64
STATE = 64
GROUPS = 2
KERNEL = 4
STRETCH = 128
SEQLEN = 4096
INNER = 7168
DOCS = 4


def aligned_pair(key):
    shape = (SEQLEN, HEADS * HEAD_DIM)
    normal_query = jax.random.truncated_normal(jax.random.fold_in(key, 11), -4.5, 4.5, shape, jnp.float32)
    normal_key = jax.random.truncated_normal(jax.random.fold_in(key, 12), -4.5, 4.5, shape, jnp.float32)
    return (normal_query, normal_key)


def draw_queries(key, part):
    return aligned_pair(key)[0].astype(jnp.bfloat16)


def draw_keys(key, part):
    return aligned_pair(key)[1].astype(jnp.bfloat16)


def draw_step_raw(key, part):
    blocks = SEQLEN // STRETCH
    offsets = jax.random.uniform(jax.random.fold_in(key, 21), (blocks, 1, SSM_HEADS), jnp.float32, -1.0, 1.0)
    noise = 0.5 * jax.random.truncated_normal(jax.random.fold_in(key, 23), -5.0, 5.0, (blocks, STRETCH, SSM_HEADS), jnp.float32)
    return (noise + offsets).reshape(SEQLEN, SSM_HEADS)


def draw_rate_log(key, part):
    chance = 0.5
    picked = jax.random.uniform(jax.random.fold_in(key, 31), (SSM_HEADS,), jnp.float32) < chance
    quick = jnp.log(jax.random.uniform(jax.random.fold_in(key, 32), (SSM_HEADS,), jnp.float32, 0.05, 0.3))
    slowly = jnp.log(jax.random.uniform(jax.random.fold_in(key, 33), (SSM_HEADS,), jnp.float32, 0.3, 2.0) / SEQLEN)
    return jnp.where(picked, quick, slowly)


def level_of(rng, shape, cuts, least, top_value):
    factor_of = 1.0
    for dim, shards_of in cuts:
        steps = jax.random.uniform(jax.random.fold_in(jax.random.fold_in(rng, 6), dim), (shards_of,), jnp.float32, least / len(cuts), top_value / len(cuts))
        factor_of = factor_of * jnp.repeat(jnp.exp(steps), shape[dim] // shards_of).reshape((-1,) + (1,) * (len(shape) - 1 - dim))
    return factor_of


def length_profile(count, total, bound, skew):
    loads = [(1 << 20) // math.isqrt(standing ** skew) + 1 for standing in range(2, count + 1)]
    rest, holding = total - bound - (count - 1), [1] * (count - 1)
    while rest > 0:
        free = [i for i in range(count - 1) if holding[i] < bound]
        whole, left = sum([loads[i] for i in free]), rest
        for i in free:
            addition = min(bound - holding[i], max(1, left * loads[i] // whole), rest)
            holding[i] = holding[i] + addition
            rest = rest - addition
    return np.array([bound] + holding)


def ragged_sizes(rng, number_of, total, reach, slope):
    if number_of == 2:
        one = jax.random.randint(rng, (), max(1, total - reach), min(reach, total - 1) + 1)
        return jnp.stack([one, total - one])
    sizes = jnp.asarray(length_profile(number_of, total, reach, slope), jnp.int32)
    twos = (number_of - 1) // 2
    giver, sink = sizes[1:1 + 2 * twos:2], sizes[2:2 + 2 * twos:2]
    margin = jnp.minimum(giver - 1, reach - sink)
    moved = jax.random.randint(jax.random.fold_in(rng, 1), (twos,), 0, 1 << 20) % (margin + 1)
    sizes = sizes.at[1:1 + 2 * twos:2].set(giver - moved).at[2:2 + 2 * twos:2].set(sink + moved)
    return sizes[jax.random.permutation(jax.random.fold_in(rng, 2), number_of)]


def bell_draw(key, shape, scale, most, split=(), kind=jnp.bfloat16):
    entries = jax.random.normal(key, shape, jnp.float32) * scale
    if len(split) > 0:
        entries = level_of(key, shape, split, -0.22, 0.18) * entries
    return jnp.clip(entries, min=-most, max=most).astype(kind)


def setup_inputs(seed: int = 0) -> dict:
    arg_keys = jax.random.split(jax.random.key(seed), 16)
    queries = draw_queries(jax.random.fold_in(arg_keys[15], 71), 0)
    keys = draw_keys(jax.random.fold_in(arg_keys[15], 71), 0)
    values = bell_draw(arg_keys[2], (SEQLEN, HEADS * HEAD_DIM), 1.0, 6.0, ((0, 16), (1, 2)))
    attn_grad = bell_draw(arg_keys[3], (SEQLEN, HEADS * HEAD_DIM), 1.0, 6.0, ((0, 16), (1, 2)))
    doc_ids = jnp.searchsorted(jnp.cumsum(ragged_sizes(arg_keys[4], DOCS, SEQLEN, SEQLEN // 2, 2)), jnp.arange(SEQLEN), side="right").astype(jnp.int32)
    conv_input = bell_draw(arg_keys[5], (SEQLEN, INNER), 1.0, 6.0, ((0, 16), (1, 2)))
    conv_weight = bell_draw(arg_keys[6], (KERNEL, INNER), KERNEL ** -0.5, 3.0, ((1, 2),), jnp.float32)
    step_raw = draw_step_raw(jax.random.fold_in(arg_keys[15], 71), 0)
    step_bias = jnp.clip(-1.5 + 1.5 * jax.random.uniform(arg_keys[8], (SSM_HEADS,), jnp.float32) ** level_of(arg_keys[8], (SSM_HEADS,), ((0, 2),), -0.2, 0.2), -1.5, 0.0)
    rate_log = draw_rate_log(jax.random.fold_in(arg_keys[15], 71), 0)
    skip_gain = jnp.clip(0.5 + 1.0 * jax.random.uniform(arg_keys[10], (SSM_HEADS,), jnp.float32) ** level_of(arg_keys[10], (SSM_HEADS,), ((0, 2),), -0.2, 0.2), 0.5, 1.5)
    input_coeff = bell_draw(arg_keys[11], (SEQLEN, GROUPS * STATE), 0.1, 0.625, ((0, 16),))
    output_coeff = bell_draw(arg_keys[12], (SEQLEN, GROUPS * STATE), 0.1, 0.625, ((0, 16),))
    gate_input = bell_draw(arg_keys[13], (SEQLEN, INNER), 1.0, 6.0, ((0, 16), (1, 2)))
    mix_grad = bell_draw(arg_keys[14], (SEQLEN, INNER), 0.25, 1.5, ((0, 16), (1, 2)))
    return dict(queries=queries, keys=keys, values=values, attn_grad=attn_grad, doc_ids=doc_ids, conv_input=conv_input, conv_weight=conv_weight, step_raw=step_raw, step_bias=step_bias, rate_log=rate_log, skip_gain=skip_gain, input_coeff=input_coeff, output_coeff=output_coeff, gate_input=gate_input, mix_grad=mix_grad)


NEG_FILL = -1e+30
EXACT = lax.Precision.HIGHEST

def conv_act(padded, doc_ext, weight):
    kernel_taps = weight.shape[0]
    length = padded.shape[0] - kernel_taps + 1
    doc_now = doc_ext[kernel_taps - 1:]
    summed = jnp.zeros((length, padded.shape[1]), jnp.float32)
    for lagged in range(kernel_taps):
        first_row = kernel_taps - 1 - lagged
        shifted = padded[first_row:first_row + length]
        same_doc = doc_ext[first_row:first_row + length] == doc_now
        summed = summed + weight[lagged] * jnp.where(same_doc[:, None], shifted, 0.0)
    return jax.nn.silu(summed)

def stretch_layout(log_decay, doc_row, doc_before):
    blocks = doc_row.shape[0] // STRETCH
    cumulative = jnp.cumsum(log_decay.reshape(blocks, STRETCH), axis=1)
    doc_grid = doc_row.reshape(blocks, STRETCH)
    previous = jnp.concatenate([jnp.reshape(doc_before, (1,)), doc_grid[:-1, -1]])
    return (cumulative, doc_grid, previous)

def head_final(head_act, step_size, log_decay, in_grid, start_state, doc_row, doc_before):
    cumulative, doc_grid, previous = stretch_layout(log_decay, doc_row, doc_before)
    blocks = cumulative.shape[0]
    scaled = (head_act * step_size[:, None]).reshape(blocks, STRETCH, head_act.shape[1])
    same_end = doc_grid == doc_grid[:, -1:]
    to_end = jnp.where(same_end, jnp.exp(jnp.where(same_end, cumulative[:, -1:] - cumulative, 0.0)), 0.0)
    local_state = jnp.einsum('cjp,cjn->cpn', scaled * to_end[:, :, None], in_grid, precision=EXACT)
    through = jnp.where(doc_grid[:, -1] == previous, jnp.exp(cumulative[:, -1]), 0.0)

    def advance(carry_state, pair_item):
        return (pair_item[0] * carry_state + pair_item[1], carry_state)
    final_state, starts = lax.scan(advance, start_state, (through, local_state))
    return (final_state, starts, cumulative, doc_grid, previous, scaled)

def head_output(head_act, step_size, log_decay, pair_grid, in_grid, out_grid, gate_part, skip_gain, start_state, doc_row, doc_before):
    final_state, starts, cumulative, doc_grid, previous, scaled = head_final(head_act, step_size, log_decay, in_grid, start_state, doc_row, doc_before)
    causal = jnp.arange(STRETCH)[:, None] >= jnp.arange(STRETCH)[None, :]
    same_doc = (doc_grid[:, :, None] == doc_grid[:, None, :]) & causal[None]
    weights = jnp.where(same_doc, jnp.exp(jnp.where(same_doc, cumulative[:, :, None] - cumulative[:, None, :], 0.0)), 0.0)
    inner_part = jnp.einsum('cij,cjp->cip', pair_grid * weights, scaled, precision=EXACT)
    enter_gain = jnp.where(doc_grid == previous[:, None], jnp.exp(cumulative), 0.0)
    carried = jnp.einsum('cin,cpn->cip', out_grid, starts, precision=EXACT) * enter_gain[:, :, None]
    mixed_out = (inner_part + carried).reshape(head_act.shape) + skip_gain * head_act
    return (mixed_out * jax.nn.silu(gate_part), final_state)

def round_edge(term):
    edge = lax.optimization_barrier(term[:WINDOW].astype(jnp.bfloat16)).astype(jnp.float32)
    return jnp.concatenate([edge, term[WINDOW:]], axis=0)

def attention_grads(queries, keys, values, attn_grad, doc_ids):
    width = HEADS * HEAD_DIM
    span = WINDOW + T_DEV
    scale = HEAD_DIM ** (-0.5)
    key_pad = jnp.concatenate([jnp.zeros((WINDOW, width), keys.dtype), keys])
    value_pad = jnp.concatenate([jnp.zeros((WINDOW, width), values.dtype), values])
    doc_pad = jnp.concatenate([jnp.full((WINDOW,), -1, jnp.int32), doc_ids])
    distance = jnp.arange(T_DEV)[:, None] + WINDOW - jnp.arange(span)[None, :]
    in_window = (distance >= 0) & (distance < WINDOW)

    def one_block(carry, index):
        key_acc, value_acc = carry
        first_row = index * T_DEV
        query_part = lax.dynamic_slice_in_dim(queries, first_row, T_DEV).astype(jnp.float32).reshape(T_DEV, HEADS, HEAD_DIM)
        grad_part = lax.dynamic_slice_in_dim(attn_grad, first_row, T_DEV).astype(jnp.float32).reshape(T_DEV, HEADS, HEAD_DIM)
        key_part = lax.dynamic_slice_in_dim(key_pad, first_row, span).astype(jnp.float32).reshape(span, HEADS, HEAD_DIM)
        value_part = lax.dynamic_slice_in_dim(value_pad, first_row, span).astype(jnp.float32).reshape(span, HEADS, HEAD_DIM)
        doc_query = lax.dynamic_slice_in_dim(doc_ids, first_row, T_DEV)
        doc_key = lax.dynamic_slice_in_dim(doc_pad, first_row, span)
        allowed = in_window & (doc_query[:, None] == doc_key[None, :])
        scores = jnp.where(allowed[None], jnp.einsum('ihd,jhd->hij', query_part, key_part) * scale, NEG_FILL)
        row_max = lax.optimization_barrier(jnp.max(scores, axis=-1))
        expo = jnp.where(allowed[None], jnp.exp(scores - row_max[:, :, None]), 0.0)
        row_sum = lax.optimization_barrier(jnp.sum(expo, axis=-1))
        probs = expo / jnp.maximum(row_sum, 1.0)[:, :, None]
        probs_half = lax.optimization_barrier(probs.astype(jnp.bfloat16)).astype(jnp.float32)
        attn_out = jnp.einsum('hij,jhd->ihd', probs_half, value_part)
        delta = lax.optimization_barrier(jnp.sum(grad_part * attn_out, axis=-1)).T
        dprob = jnp.einsum('ihd,jhd->hij', grad_part, value_part)
        dscore = lax.optimization_barrier((probs * (dprob - delta[:, :, None])).astype(jnp.bfloat16)).astype(jnp.float32)
        grad_query = (jnp.einsum('hij,jhd->ihd', dscore, key_part) * scale).reshape(T_DEV, width).astype(jnp.bfloat16)
        key_term = round_edge(jnp.einsum('hij,ihd->jhd', dscore, query_part).reshape(span, width))
        value_term = round_edge(jnp.einsum('hij,ihd->jhd', probs_half, grad_part).reshape(span, width))
        key_acc = lax.dynamic_update_slice_in_dim(key_acc, lax.dynamic_slice_in_dim(key_acc, first_row, span) + key_term, first_row, 0)
        value_acc = lax.dynamic_update_slice_in_dim(value_acc, lax.dynamic_slice_in_dim(value_acc, first_row, span) + value_term, first_row, 0)
        return ((key_acc, value_acc), grad_query)
    zero_acc = jnp.zeros((WINDOW + SEQLEN, width), jnp.float32)
    (key_acc, value_acc), grad_blocks = lax.scan(one_block, (zero_acc, zero_acc), jnp.arange(SEQLEN // T_DEV, dtype=jnp.int32))
    grad_queries = grad_blocks.reshape(SEQLEN, width)
    grad_keys = (key_acc[WINDOW:] * scale).astype(jnp.bfloat16)
    grad_values = value_acc[WINDOW:].astype(jnp.bfloat16)
    return (grad_queries, grad_keys, grad_values)

def mixer_grads(doc_ids, conv_input, conv_weight, step_raw, step_bias, rate_log, skip_gain, input_coeff, output_coeff, gate_input, mix_grad):
    doc_ext = jnp.concatenate([jnp.full((KERNEL - 1,), -1, jnp.int32), doc_ids])
    padded_all = jnp.concatenate([jnp.zeros((KERNEL - 1, INNER), jnp.float32), conv_input.astype(jnp.float32)])
    group_heads = SSM_HEADS // GROUPS
    blocks = SEQLEN // STRETCH
    zero_state = jnp.zeros((SSM_DIM, STATE), jnp.float32)
    start_doc = jnp.int32(-1)

    def forward(padded, weight, raw_step, bias_one, rate_one, skip_one, group_in, group_out, gate_part):
        head_act = conv_act(padded, doc_ext, weight)
        step_size = jax.nn.softplus(raw_step + bias_one)
        log_decay = -step_size * jnp.exp(rate_one)
        in_grid = group_in.reshape(blocks, STRETCH, STATE)
        out_grid = group_out.reshape(blocks, STRETCH, STATE)
        pair_grid = jnp.einsum('cin,cjn->cij', out_grid, in_grid, precision=EXACT)
        return head_output(head_act, step_size, log_decay, pair_grid, in_grid, out_grid, gate_part, skip_one, zero_state, doc_ids, start_doc)[0]

    def one_head(carry, head_index):
        sum_in, sum_out = carry
        column = head_index * SSM_DIM
        group_col = head_index // group_heads * STATE
        primals = (lax.dynamic_slice_in_dim(padded_all, column, SSM_DIM, 1), lax.dynamic_slice_in_dim(conv_weight, column, SSM_DIM, 1), lax.dynamic_index_in_dim(step_raw, head_index, 1, keepdims=False), step_bias[head_index], rate_log[head_index], skip_gain[head_index], lax.dynamic_slice_in_dim(input_coeff, group_col, STATE, 1).astype(jnp.float32), lax.dynamic_slice_in_dim(output_coeff, group_col, STATE, 1).astype(jnp.float32), lax.dynamic_slice_in_dim(gate_input, column, SSM_DIM, 1).astype(jnp.float32))
        cotangent = lax.dynamic_slice_in_dim(mix_grad, column, SSM_DIM, 1).astype(jnp.float32)
        gradients = jax.vjp(forward, *primals)[1](cotangent)
        sum_in = lax.dynamic_update_slice_in_dim(sum_in, lax.dynamic_slice_in_dim(sum_in, group_col, STATE, 1) + gradients[6], group_col, 1)
        sum_out = lax.dynamic_update_slice_in_dim(sum_out, lax.dynamic_slice_in_dim(sum_out, group_col, STATE, 1) + gradients[7], group_col, 1)
        return ((sum_in, sum_out), (gradients[0][KERNEL - 1:].astype(jnp.bfloat16), gradients[8].astype(jnp.bfloat16), gradients[2], gradients[1], gradients[3], gradients[4], gradients[5]))
    zero_cols = jnp.zeros((SEQLEN, GROUPS * STATE), jnp.float32)
    (sum_in, sum_out), stacked = lax.scan(one_head, (zero_cols, zero_cols), jnp.arange(SSM_HEADS, dtype=jnp.int32))
    conv_grad, gate_grad, step_grad, weight_grad, bias_grad, rate_grad, skip_grad = stacked
    grad_conv_input = jnp.transpose(conv_grad, (1, 0, 2)).reshape(SEQLEN, INNER)
    grad_gate = jnp.transpose(gate_grad, (1, 0, 2)).reshape(SEQLEN, INNER)
    grad_conv_weight = jnp.transpose(weight_grad, (1, 0, 2)).reshape(KERNEL, INNER)
    return (grad_conv_input, grad_gate, step_grad.T, sum_in, sum_out, grad_conv_weight, bias_grad, rate_grad, skip_grad)

def reference(queries, keys, values, attn_grad, doc_ids, conv_input, conv_weight, step_raw, step_bias, rate_log, skip_gain, input_coeff, output_coeff, gate_input, mix_grad):
    grad_queries, grad_keys, grad_values = attention_grads(queries, keys, values, attn_grad, doc_ids)
    grad_conv_input, grad_gate, grad_step, grad_input_coeff, grad_output_coeff, grad_conv_weight, grad_step_bias, grad_rate_log, grad_skip = mixer_grads(doc_ids, conv_input, conv_weight, step_raw, step_bias, rate_log, skip_gain, input_coeff, output_coeff, gate_input, mix_grad)
    return (grad_queries, grad_keys, grad_values, grad_conv_input, grad_gate, grad_step, grad_input_coeff, grad_output_coeff, grad_conv_weight, grad_step_bias, grad_rate_log, grad_skip)
```

```python
import functools
import types

import jax
import jax.numpy as jnp
from jax import lax
from jax.experimental import pallas as pl
from jax.experimental.pallas import tpu as pltpu
from jax.sharding import PartitionSpec as P

HEAD_DIM = 224
WIDE = 256
WINDOW = 1024
SSM_HEADS = 112
STATE = 64
GROUPS = 2
KERNEL = 4
PAD = 8
EDGE = 16
LANES = 128

EXACT = lax.Precision.HIGHEST
F32 = jnp.float32
BF16 = jnp.bfloat16
NEG_FILL = -1e30
SCALE = HEAD_DIM ** (-0.5)
MESH = pl.DeviceIdType.MESH


def dot(a, b, ca, cb, precision=None):
    return lax.dot_general(
        a, b, (((ca,), (cb,)), ((), ())), preferred_element_type=F32, precision=precision
    )


def aligned(first, size):
    return pl.ds(pl.multiple_of(first, size), size)


def iota(shape, dim):
    return lax.broadcasted_iota(jnp.int32, shape, dim)


class Exchange:
    def __init__(self, make, offsets):
        self.make, self.offsets = make, offsets

    def start(self):
        for d in self.offsets:
            self.make(d).start()

    def wait_recv(self):
        for d in self.offsets:
            self.make(d).wait_recv()

    def wait_send(self):
        for d in self.offsets:
            self.make(d).wait_send()


def remote(src, dst, sems, where, **device):
    return pltpu.make_async_remote_copy(
        src_ref=src, dst_ref=dst, send_sem=sems[0].at[where], recv_sem=sems[1].at[where],
        device_id=device, device_id_type=MESH,
    )


def expand(values, index):
    return jnp.take_along_axis(values, index, axis=1, mode="promise_in_bounds")


def turned(value):
    return value.astype(F32).T


def kernel(z, *refs):
    r = types.SimpleNamespace(**dict(zip(z.names, refs)))
    R, C, H, Hs, G = z.rows, z.channels, z.heads, z.ssm_heads, z.group
    per, span, CW = z.per, z.group * z.rows, z.chunk * LANES
    index = lax.axis_index("seq")
    head = lax.axis_index("head")
    place = lax.rem(index, G)
    base = index - place
    plane = lax.div(index, G)
    part = lax.div(head * Hs, SSM_HEADS // GROUPS)
    others = range(1, G)
    has_next, has_prev = index + G < z.count, index >= G

    def to_place(d):
        return lax.rem(place + d, G)

    def from_place(d):
        return lax.rem(place + G - d, G)

    def ring(at):
        return lax.rem(at + z.count, z.count)

    def kv_out(hh, d):
        p = to_place(d)
        return remote(
            r.send.at[per * p + hh, pl.ds(0, 2)], r.kv.at[hh, :, aligned(span + place * R, R)],
            (r.kv_s, r.kv_r), (hh, d), seq=base + p,
        )

    def qd_out(hh, d):
        p = to_place(d)
        return remote(
            r.send.at[per * p + hh, pl.ds(2, 2)], r.qd.at[hh, :, aligned(place * R, R)],
            (r.qd_s, r.qd_r), (hh, d), seq=base + p,
        )

    def forward(hh, d):
        p = from_place(d)
        return remote(
            r.kv.at[hh, :, aligned(span + p * R, R)], r.kv.at[hh, :, aligned(p * R, R)],
            (r.fw_s, r.fw_r), (hh, d), seq=ring(index + G),
        )

    def backward(hh, b):
        return remote(
            r.bks.at[hh, :, aligned(b * R, R)], r.bkr.at[hh, :, aligned(b * R, R)],
            (r.bk_s, r.bk_r), (hh, b), seq=ring(index - G),
        )

    def dq_out(hh, d):
        p = to_place(d)
        return remote(
            r.dq.at[hh, aligned(p * R, R)], r.fin.at[per * place + hh, 0],
            (r.dq_s, r.dq_r), (hh, d), seq=base + p,
        )

    def dkv_out(hh, d):
        p = to_place(d)
        return remote(
            r.kvo.at[hh, :, aligned(p * R, R)], r.fin.at[per * place + hh, pl.ds(1, 2)],
            (r.do_s, r.do_r), (hh, d), seq=base + p,
        )

    def tail_out():
        return remote(
            r.conv.at[pl.ds(R - EDGE, EDGE)], r.tail, (r.one_s, r.one_r), 0, seq=ring(index + 1)
        )

    def spill_out():
        return remote(r.edge, r.spill, (r.one_s, r.one_r), 1, seq=ring(index - 1))

    def state_out(d):
        p = to_place(d)
        return remote(r.st_s.at[p], r.st_a.at[place], (r.st_ss, r.st_sr), d, seq=base + p)

    def decay_out(d):
        p = to_place(d)
        return remote(r.th_s.at[p], r.th_a.at[place], (r.th_ss, r.th_sr), d, seq=base + p)

    def up_out(k):
        return remote(r.agg.at[0], r.up.at[k], (r.up_s, r.up_r), k, seq=ring(index + k * G))

    def up_decay(k):
        return remote(r.aggt, r.upt.at[k], (r.ut_s, r.ut_r), k, seq=ring(index + k * G))

    def down_out(k):
        return remote(r.agg.at[1], r.dn.at[k], (r.dn_s, r.dn_r), k, seq=ring(index - k * G))

    def down_decay(k):
        return remote(r.aggt, r.dnt.at[k], (r.dt_s, r.dt_r), k, seq=ring(index - k * G))

    def enter_out(d):
        p = to_place(d)
        return remote(r.ent_s.at[p], r.ent.at[place], (r.en_s, r.en_r), d, seq=base + p)

    def sum_out(d):
        p = to_place(d)
        return remote(r.red_s.at[p], r.red_a.at[place], (r.ra_s, r.ra_r), d, seq=base + p)

    def plane_out(k):
        return remote(
            r.red_p, r.red_z.at[plane], (r.rz_s, r.rz_r), k, seq=ring(index + k * G)
        )

    def total_out(d):
        return remote(r.red_t, r.red_o.at[place], (r.ro_s, r.ro_r), d, seq=base + to_place(d))

    def coeff_out(d):
        return remote(
            r.co_s, r.co_a.at[head], (r.co_ss, r.co_sr), d, head=lax.rem(head + d, z.head_count)
        )

    head_others = range(1, z.head_count)
    planes = z.count // G
    reach = range(1, z.reach + 1)

    @pl.when(index + 1 < z.count)
    def _():
        tail_out().start()

    @pl.when(index == 0)
    def _():
        r.tail[...] = jnp.zeros_like(r.tail)

    def window(h, ref):
        first = h * HEAD_DIM // LANES * LANES
        last = -(-(h + 1) * HEAD_DIM // LANES) * LANES
        return first, last, h * HEAD_DIM - first

    def pack(ref, h, a):
        first, last, off = window(h, ref)
        value = ref[:, first:last].astype(F32)
        if off:
            value = pltpu.roll(value, last - first - off, 1)
        value = value[:, :WIDE]
        keep = iota((R, WIDE), 1) < HEAD_DIM
        r.send[h, a] = jnp.where(keep, value, 0.0).astype(BF16)

    def own_piece(hh):
        mine = per * place + hh
        for a in range(2):
            r.kv[hh, a, aligned(span + place * R, R), :] = r.send[mine, a]
            r.qd[hh, a, aligned(place * R, R), :] = r.send[mine, 2 + a]

    for h in range(H):
        for a, ref in enumerate((r.k, r.v, r.q, r.do)):
            pack(ref, h, a)
    for hh in range(per):
        for d in others:
            kv_out(hh, d).start()
        for d in others:
            qd_out(hh, d).start()
    for hh in range(per):
        own_piece(hh)

    @pl.when(has_next)
    def _():
        for hh in range(per):
            forward(hh, 0).start()

    @pl.when(jnp.logical_not(has_prev))
    def _():
        for hh in range(per):
            for a in range(2):
                r.kv[hh, a, pl.ds(0, span), :] = jnp.zeros((span, WIDE), BF16)

    @pl.when(jnp.logical_not(has_next))
    def _():
        r.bkr[...] = jnp.zeros_like(r.bkr)

    def pass_on(hh, d):
        kv_out(hh, d).wait_recv()

        @pl.when(has_next)
        def _():
            forward(hh, d).start()

    for t in range(2 * G):
        row = r.docs[pl.ds(base + t, 1), :]
        r.dcol[t * R : (t + 1) * R, :] = jnp.broadcast_to(row, (LANES, R)).T
    own_doc = span + place * R
    r.mext[...] = r.dcol[pl.ds(pl.multiple_of(own_doc - PAD, PAD), R + PAD), :]
    doc_now = r.mext[PAD:, :]
    for lag in range(1, KERNEL):
        r.mask[lag - 1] = (r.mext[PAD - lag : PAD - lag + R, :] == doc_now).astype(F32)
    i2, j2 = iota((R, R), 0), iota((R, R), 1)
    doc_row = r.docs[pl.ds(index + G, 1), :]
    doc_pair = jnp.concatenate([doc_now] * (R // LANES), axis=1)
    r.bias[...] = jnp.where((i2 >= j2) & (doc_pair == doc_row), 0.0, NEG_FILL)

    r.raw[...] = jnp.zeros_like(r.raw)
    r.raw[:, :Hs] = r.step_raw[...] + r.step_bias[...]
    r.head_rows[...] = jnp.zeros_like(r.head_rows)
    r.head_rows[0:1, :Hs] = jnp.exp(r.rate_log[...])
    r.head_rows[1:2, :Hs] = r.skip_gain[...]
    raw = r.raw[...]
    rate = r.head_rows[0:1, :]
    size_all = jnp.maximum(raw, 0.0) + jnp.log1p(jnp.exp(-jnp.abs(raw)))
    log_decay = -size_all * rate
    tri = (i2 >= j2).astype(F32)
    cum = dot(tri, log_decay, 1, 0, EXACT)
    enter_all = jnp.where(doc_now == r.mext[PAD - 1 : PAD, :], jnp.exp(cum), 0.0)
    to_end_all = jnp.where(
        doc_now == r.mext[R + PAD - 1 : R + PAD, :], jnp.exp(cum[R - 1 : R, :] - cum), 0.0
    )
    r.cum[...] = cum
    r.cumt[...] = cum.T
    r.size[...] = size_all
    r.enter[...] = enter_all
    r.to_end[...] = to_end_all

    b_wide, c_wide = r.b_in[...], r.c_in[...]
    b_own, c_own = b_wide[:, :STATE], c_wide[:, :STATE]
    for g in range(1, GROUPS):
        b_own = jnp.where(part == g, b_wide[:, g * STATE : (g + 1) * STATE], b_own)
        c_own = jnp.where(part == g, c_wide[:, g * STATE : (g + 1) * STATE], c_own)
    r.b[...] = b_own
    r.c[...] = c_own
    r.bt[...] = turned(b_own).astype(BF16)
    r.ct[...] = turned(c_own).astype(BF16)
    r.pair[...] = dot(c_own, b_own, 1, 1)

    @pl.when(index > 0)
    def _():
        tail_out().wait_recv()

    lower = iota((R, LANES), 1) < LANES // 2
    half = jnp.where(lower, 0, 1)

    def conv_pre(lanes):
        r.xp[:PAD, :] = r.tail[:, lanes].astype(F32)[EDGE - PAD :, :]
        r.xp[PAD:, :] = r.conv[:, lanes].astype(F32)
        pre = r.cw[0:1, lanes] * r.xp[PAD:, :]
        for lag in range(1, KERNEL):
            pre = pre + r.cw[lag : lag + 1, lanes] * (
                r.xp[PAD - lag : PAD - lag + R, :] * r.mask[lag - 1]
            )
        return pre

    def ends(c):
        def one(m, carry):
            p = c * z.chunk + m
            lanes = aligned(p * LANES, LANES)
            here = aligned(m * LANES, LANES)
            pre = conv_pre(lanes)
            act = pre * jax.nn.sigmoid(pre)
            who = half + 2 * p
            enter = expand(r.enter[...], who)
            weighted = act * expand(r.size[...], who) * expand(r.to_end[...], who)
            r.st_s[c, 0, :, here] = dot(r.bt[...], weighted.astype(BF16), 1, 0).astype(BF16)
            gate = r.gate[:, lanes].astype(F32)
            dy = r.mix[:, lanes].astype(F32) * (gate * jax.nn.sigmoid(gate))
            r.st_s[c, 1, :, here] = dot(r.ct[...], (dy * enter).astype(BF16), 1, 0).astype(BF16)
            r.th_s[c, :, here] = jnp.broadcast_to(enter[R - 1 : R, :], (PAD, LANES))
            return carry

        lax.fori_loop(0, z.chunks[c], one, 0)

    if z.padded:
        r.st_s[...] = jnp.zeros_like(r.st_s)
        r.th_s[...] = jnp.zeros_like(r.th_s)
        r.red_s[...] = jnp.zeros_like(r.red_s)

    for c in range(G):
        ends(c)
        if c > 0:
            pass_on(0, c)
    state, decay = Exchange(state_out, others), Exchange(decay_out, others)
    state.start()
    decay.start()
    r.st_a[place] = r.st_s[place]
    r.th_a[place] = r.th_s[place]

    r.dkv[...] = jnp.zeros_like(r.dkv)

    def attention(hh):
        j, i = iota((R, R), 0), iota((R, R), 1)

        def block(b, carry):
            mine = aligned(b * R, R)
            q = r.qd[hh, 0, mine, :]
            grad = r.qd[hh, 1, mine, :]
            docq = r.docs[pl.ds(base + G + b, 1), :]
            places = [aligned((b + G - gap) * R, R) for gap in range(G + 1)]
            scores = []
            top = None
            for gap in range(G + 1):
                dock = r.dcol[places[gap], :]
                allowed = jnp.concatenate([dock] * (R // LANES), axis=1) == docq
                if gap == 0:
                    allowed = allowed & (i >= j)
                if gap == G:
                    allowed = allowed & (i < j)
                s = jnp.where(allowed, dot(r.kv[hh, 0, places[gap], :], q, 1, 1) * SCALE, NEG_FILL)
                scores.append(s)
                m = jnp.max(s, axis=0, keepdims=True)
                top = m if top is None else jnp.maximum(top, m)
            total = None
            expo = []
            for gap in range(G + 1):
                e = jnp.exp(scores[gap] - top)
                expo.append(e)
                t = jnp.sum(e, axis=0, keepdims=True)
                total = t if total is None else total + t
            inverse = 1.0 / jnp.maximum(total, 1.0)
            delta = None
            dprobs = []
            for gap in range(G + 1):
                weight = (expo[gap] * inverse).astype(BF16)
                dp = dot(r.kv[hh, 1, places[gap], :], grad, 1, 1)
                d = jnp.sum(weight.astype(F32) * dp, axis=0, keepdims=True)
                delta = d if delta is None else delta + d
                r.dkv[hh, 1, places[gap], :] += dot(weight, grad, 1, 0)
                dprobs.append(dp)
            dq = None
            for gap in range(G + 1):
                ds = (expo[gap] * inverse * (dprobs[gap] - delta)).astype(BF16)
                r.dkv[hh, 0, places[gap], :] += dot(ds, q, 1, 0)
                piece = dot(ds, r.kv[hh, 0, places[gap], :], 0, 0)
                dq = piece if dq is None else dq + piece
            r.dq[hh, mine, :] = (dq * SCALE).astype(BF16)

            @pl.when(has_prev)
            def _():
                for a in range(2):
                    r.bks[hh, a, mine, :] = r.dkv[hh, a, mine, :].astype(BF16)
                backward(hh, b).start()

            return carry

        lax.fori_loop(0, G, block, 0)
        for d in others:
            dq_out(hh, d).start()
        r.fin[per * place + hh, 0] = r.dq[hh, aligned(place * R, R), :]

    def attention_inputs(hh):
        for d in others:
            qd_out(hh, d).wait_recv()

        @pl.when(has_prev)
        def _():
            for d in range(G):
                forward(hh, d).wait_recv()

    def give_back(hh):
        @pl.when(has_next)
        def _():
            for b in range(G):
                backward(hh, b).wait_recv()

        for t in range(G):
            rows = slice(t * R, (t + 1) * R)
            own = slice(span + t * R, span + (t + 1) * R)
            dk = (r.dkv[hh, 0, own, :] + r.bkr[hh, 0, rows, :].astype(F32)) * SCALE
            dv = r.dkv[hh, 1, own, :] + r.bkr[hh, 1, rows, :].astype(F32)
            r.kvo[hh, 0, rows, :] = dk.astype(BF16)
            r.kvo[hh, 1, rows, :] = dv.astype(BF16)
        for d in others:
            dkv_out(hh, d).start()
        for a in range(2):
            r.fin[per * place + hh, 1 + a] = r.kvo[hh, a, aligned(place * R, R), :]

    def tall(rows):
        return jnp.concatenate([rows] * (STATE // PAD), axis=0)

    def through(t, here):
        return tall(r.th_a[t, :, here])

    def chain_out():
        state.wait_recv()
        decay.wait_recv()
        def one(m, carry):
            here = aligned(m * LANES, LANES)
            a = r.st_a[0, 0, :, here].astype(F32)
            thr = r.th_a[0, :, here]
            for t in range(1, G):
                a = a * through(t, here) + r.st_a[t, 0, :, here].astype(F32)
                thr = thr * r.th_a[t, :, here]
            b = r.st_a[G - 1, 1, :, here].astype(F32)
            for t in range(G - 2, -1, -1):
                b = b * through(t, here) + r.st_a[t, 1, :, here].astype(F32)
            r.agg[0, :, here] = a.astype(BF16)
            r.agg[1, :, here] = b.astype(BF16)
            r.aggt[:, here] = thr
            return carry

        lax.fori_loop(0, z.chunk, one, 0)
        for k in reach:
            @pl.when(index + k * G < z.count)
            def _():
                up_out(k).start()
                up_decay(k).start()

            @pl.when(index + k * G >= z.count)
            def _():
                r.dn[k] = jnp.zeros((STATE, CW), BF16)
                r.dnt[k] = jnp.zeros((PAD, CW), F32)

            @pl.when(index - k * G >= 0)
            def _():
                down_out(k).start()
                down_decay(k).start()

            @pl.when(index - k * G < 0)
            def _():
                r.up[k] = jnp.zeros((STATE, CW), BF16)
                r.upt[k] = jnp.zeros((PAD, CW), F32)

    def chain_in():
        for k in reach:
            @pl.when(index - k * G >= 0)
            def _():
                up_out(k).wait_recv()
                up_decay(k).wait_recv()

            @pl.when(index + k * G < z.count)
            def _():
                down_out(k).wait_recv()
                down_decay(k).wait_recv()

        def one(m, carry):
            here = aligned(m * LANES, LANES)
            s = jnp.zeros((STATE, LANES), F32)
            e = jnp.zeros((STATE, LANES), F32)
            for k in reversed(reach):
                s = s * tall(r.upt[k, :, here]) + r.up[k, :, here].astype(F32)
                e = e * tall(r.dnt[k, :, here]) + r.dn[k, :, here].astype(F32)
            for t in range(G):
                r.ent_s[t, 0, :, here] = s.astype(BF16)
                s = s * through(t, here) + r.st_a[t, 0, :, here].astype(F32)
            for t in range(G - 1, -1, -1):
                r.ent_s[t, 1, :, here] = e.astype(BF16)
                e = e * through(t, here) + r.st_a[t, 1, :, here].astype(F32)
            return carry

        lax.fori_loop(0, z.chunk, one, 0)
        for d in others:
            enter_out(d).start()
        r.ent[place] = r.ent_s[place]

    r.dpair[...] = jnp.zeros_like(r.dpair)
    r.db[...] = jnp.zeros_like(r.db)
    r.dc[...] = jnp.zeros_like(r.dc)
    r.zsum[...] = jnp.zeros_like(r.zsum)
    r.usum[...] = jnp.zeros_like(r.usum)
    r.acc[...] = jnp.zeros_like(r.acc)
    r.dpad[...] = jnp.zeros_like(r.dpad)
    lane = iota((R, LANES), 1)
    lane_row = iota((PAD, LANES), 1)

    def mixer(c):
        def one(m, carry):
            p = c * z.chunk + m
            lanes = aligned(p * LANES, LANES)
            here = aligned(m * LANES, LANES)
            who = half + 2 * p
            size = expand(r.size[...], who)
            enter = expand(r.enter[...], who)
            to_end = expand(r.to_end[...], who)
            pre = conv_pre(lanes)
            sig_pre = jax.nn.sigmoid(pre)
            act = pre * sig_pre
            x_half = (act * size).astype(BF16)
            gate = r.gate[:, lanes].astype(F32)
            sig_gate = jax.nn.sigmoid(gate)
            silu_gate = gate * sig_gate
            cot = r.mix[:, lanes].astype(F32)
            dy = cot * silu_gate
            dy_half = dy.astype(BF16)
            state_in = r.ent[c, 0, :, here]
            end_cot = r.ent[c, 1, :, here]
            zero = jnp.zeros_like(dy_half)
            y_parts, dx_parts = [], []
            dpair = r.dpair[...]
            for k in range(2):
                column = expand(r.cum[...], jnp.zeros((R, LANES), jnp.int32) + (2 * p + k))
                column = jnp.concatenate([column] * (R // LANES), axis=1)
                weights = jnp.exp((column - r.cumt[pl.ds(2 * p + k, 1), :]) + r.bias[...])
                mixing = (r.pair[...] * weights).astype(BF16)
                y_parts.append(dot(mixing, x_half, 1, 0))
                dx_parts.append(dot(mixing, dy_half, 0, 0))
                dy_one = jnp.where(lower if k == 0 else ~lower, dy_half, zero)
                dpair = dpair + dot(dy_one, x_half, 1, 1) * weights
            r.dpair[...] = dpair
            inner = jnp.where(lower, y_parts[0], y_parts[1]) + enter * dot(r.c[...], state_in, 1, 0)
            end_part = to_end * dot(r.b[...], end_cot, 1, 0)
            dx = jnp.where(lower, dx_parts[0], dx_parts[1]) + end_part
            skip = expand(jnp.broadcast_to(r.head_rows[1:2, :], (PAD, LANES)), who[:PAD])[0:1]
            y = inner + skip * act
            r.ggate[:, lanes] = (cot * y * (sig_gate + silu_gate * (1.0 - sig_gate))).astype(BF16)
            x_wide = x_half.astype(F32)
            zed = dy_half.astype(F32) * inner - x_wide * dx
            you = dx * act
            r.dc[...] += dot((enter * dy).astype(BF16), state_in, 1, 1)
            r.db[...] += dot((to_end * x_wide).astype(BF16), end_cot, 1, 1)
            dact = dx * size + skip * dy
            dpre = dact * (sig_pre + act * (1.0 - sig_pre))
            sums = [jnp.sum(dpre * r.xp[PAD:, :], axis=0, keepdims=True)]
            r.dpad[0, PAD : PAD + R, :] = dpre
            grown = r.cw[0:1, lanes] * r.dpad[0, 0 : R + PAD, :]
            for lag in range(1, KERNEL):
                masked = dpre * r.mask[lag - 1]
                sums.append(
                    jnp.sum(masked * r.xp[PAD - lag : PAD - lag + R, :], axis=0, keepdims=True)
                )
                r.dpad[lag, PAD : PAD + R, :] = masked
                grown = grown + r.cw[lag : lag + 1, lanes] * r.dpad[lag, lag : lag + R + PAD, :]
            r.gconv[:, lanes] = grown[PAD:, :].astype(BF16)
            r.edge[:, lanes] = grown[:PAD, :]
            r.keep[:, lanes] = grown[R + PAD - EDGE :, :]
            none = jnp.zeros((PAD - KERNEL, LANES), F32)
            r.red_s[c, :, here] = jnp.concatenate(sums + [none], axis=0)
            heads3 = jnp.concatenate(
                [
                    jnp.sum(dy * act, axis=0, keepdims=True),
                    jnp.sum(state_in.astype(F32) * end_cot.astype(F32), axis=0, keepdims=True),
                    jnp.sum(x_wide * end_part, axis=0, keepdims=True),
                    jnp.zeros((PAD - 3, LANES), F32),
                ],
                axis=0,
            )
            for k in range(2):
                side = lower if k == 0 else ~lower
                mine = lane == 2 * p + k
                z_one = jnp.sum(jnp.where(side, zed, 0.0), axis=1, keepdims=True)
                u_one = jnp.sum(jnp.where(side, you, 0.0), axis=1, keepdims=True)
                h_one = jnp.sum(jnp.where(side[:PAD], heads3, 0.0), axis=1, keepdims=True)
                r.zsum[...] = jnp.where(mine, z_one, r.zsum[...])
                r.usum[...] = jnp.where(mine, u_one, r.usum[...])
                r.acc[...] = jnp.where(lane_row == 2 * p + k, h_one, r.acc[...])
            return carry

        lax.fori_loop(0, z.chunks[c], one, 0)

    def mixer_start():
        for d in others:
            enter_out(d).wait_recv()

    def mixer_end():
        @pl.when(index > 0)
        def _():
            spill_out().start()

        total = r.dpair[...]
        dc = r.dc[...] + dot(total, r.b[...].astype(F32), 1, 0, EXACT)
        db = r.db[...] + dot(total, r.c[...].astype(F32), 0, 0, EXACT)
        mine = lax.div(lane, STATE) == part
        r.co_s[0] = jnp.where(mine, jnp.concatenate([db] * GROUPS, axis=1), 0.0)
        r.co_s[1] = jnp.where(mine, jnp.concatenate([dc] * GROUPS, axis=1), 0.0)
        for d in head_others:
            coeff_out(d).start()
        r.co_a[head] = r.co_s[...]
        last_row = r.acc[2:3, :] + r.enter[R - 1 : R, :] * r.acc[1:2, :]
        rows = iota((R, LANES), 0)
        dcum = r.zsum[...] + jnp.where(rows == R - 1, last_row, 0.0)
        upper = (iota((R, R), 0) <= iota((R, R), 1)).astype(F32)
        dlog = dot(upper, dcum, 1, 0, EXACT)
        rates = r.head_rows[0:1, :]
        grad_step = (r.usum[...] - dlog * rates) * jax.nn.sigmoid(r.raw[...])
        r.gstep[...] = grad_step[:, :Hs]
        small = jnp.concatenate(
            [
                jnp.zeros((KERNEL, LANES), F32),
                jnp.sum(grad_step, axis=0, keepdims=True),
                jnp.sum(dlog * (-r.size[...] * rates), axis=0, keepdims=True),
                r.acc[0:1, :],
                jnp.zeros((1, LANES), F32),
            ],
            axis=0,
        )
        r.red_s[0, :, 0:LANES] += small
        for d in others:
            sum_out(d).start()
        r.red_a[place] = r.red_s[place]

    def sums_planes():
        for d in others:
            sum_out(d).wait_recv()
        total = r.red_a[0]
        for t in range(1, G):
            total = total + r.red_a[t]
        r.red_p[...] = total
        for k in range(1, planes):
            plane_out(k).start()
        r.red_z[plane] = total

    def sums_all():
        for k in range(1, planes):
            plane_out(k).wait_recv()
        total = r.red_z[0]
        for t in range(1, planes):
            total = total + r.red_z[t]
        r.red_t[...] = total
        for d in others:
            total_out(d).start()
        r.red_o[place] = total

    def sums_end():
        for d in others:
            total_out(d).wait_recv()
        for c in range(G):
            width = z.chunks[c] * LANES
            if width:
                r.gcw[:, c * CW : c * CW + width] = r.red_o[c, 0:KERNEL, 0:width]
        r.small[...] = r.red_o[0, :, 0:LANES]
        for d in head_others:
            coeff_out(d).wait_recv()
        db, dc = r.co_a[0, 0], r.co_a[0, 1]
        for d in head_others:
            db = db + r.co_a[d, 0]
            dc = dc + r.co_a[d, 1]
        r.gb[...] = db
        r.gc[...] = dc

        @pl.when(index + 1 < z.count)
        def _():
            spill_out().wait_recv()

        @pl.when(index + 1 >= z.count)
        def _():
            r.spill[...] = jnp.zeros_like(r.spill)

        spill = jnp.concatenate([jnp.zeros((EDGE - PAD, C), F32), r.spill[...]], axis=0)
        r.gconv[R - EDGE :, :] = (r.keep[...] + spill).astype(BF16)

    def unpack():
        for hh in range(per):
            for d in others:
                dq_out(hh, d).wait_recv()
                dkv_out(hh, d).wait_recv()
        for a, ref in enumerate((r.gq, r.gk, r.gv)):
            open_tile = None
            for h in range(H):
                first, last, off = window(h, ref)
                value = r.fin[h, a].astype(F32)
                if last - first > WIDE:
                    value = jnp.concatenate([value, jnp.zeros((R, LANES), F32)], axis=1)
                if off:
                    value = pltpu.roll(value, off, 1)
                tiles = [value[:, n : n + LANES] for n in range(0, last - first, LANES)]
                if off:
                    tiles[0] = tiles[0] + open_tile
                done = (h + 1) * HEAD_DIM % LANES == 0
                for n, tile in enumerate(tiles if done else tiles[:-1]):
                    ref[:, first + n * LANES : first + (n + 1) * LANES] = tile.astype(BF16)
                open_tile = tiles[-1]

    for hh in range(1, per):
        for d in others:
            pass_on(hh, d)
    attention_inputs(0)
    attention(0)
    chain_out()
    for hh in range(1, per):
        attention_inputs(hh)
        attention(hh)
    chain_in()
    mixer_start()
    for c in range(G):
        mixer(c)
        if c < per:
            give_back(c)
    for hh in range(G, per):
        give_back(hh)
    mixer_end()
    sums_planes()
    unpack()
    sums_all()
    sums_end()

    for hh in range(per):
        for d in others:
            kv_out(hh, d).wait_send()
            qd_out(hh, d).wait_send()
            dq_out(hh, d).wait_send()
            dkv_out(hh, d).wait_send()

    @pl.when(has_next)
    def _():
        for hh in range(per):
            for d in range(G):
                forward(hh, d).wait_send()

    @pl.when(has_prev)
    def _():
        for hh in range(per):
            for b in range(G):
                backward(hh, b).wait_send()

    state.wait_send()
    decay.wait_send()
    for d in others:
        enter_out(d).wait_send()
        sum_out(d).wait_send()
        total_out(d).wait_send()
    for k in range(1, planes):
        plane_out(k).wait_send()
    for d in head_others:
        coeff_out(d).wait_send()
    for k in reach:
        @pl.when(index + k * G < z.count)
        def _():
            up_out(k).wait_send()
            up_decay(k).wait_send()

        @pl.when(index - k * G >= 0)
        def _():
            down_out(k).wait_send()
            down_decay(k).wait_send()

    @pl.when(index + 1 < z.count)
    def _():
        tail_out().wait_send()

    @pl.when(index > 0)
    def _():
        spill_out().wait_send()


def local(
    queries, keys, values, attn_grad, doc_ids, conv_input, conv_weight, step_raw, step_bias,
    rate_log, skip_gain, input_coeff, output_coeff, gate_input, mix_grad,
):
    rows, width = queries.shape
    channels = conv_input.shape[1]
    ssm_heads = step_raw.shape[1]
    heads = width // HEAD_DIM
    count, head_count = lax.axis_size("seq"), lax.axis_size("head")
    group = WINDOW // rows
    pairs = channels // LANES
    chunk = -(-pairs // group)
    chunks = [max(0, min(chunk, pairs - c * chunk)) for c in range(group)]
    per = heads // group
    span, cw, planes = group * rows, chunk * LANES, count // group
    reach = max(1, min(planes - 1, -(-(count // 2) // group)))
    docs = jnp.pad(doc_ids.astype(F32), (span, 0), constant_values=-1.0).reshape(count + group, rows)

    vm, dma = pltpu.VMEM, pltpu.SemaphoreType.DMA
    inputs = dict(
        q=queries, k=keys, v=values, do=attn_grad, docs=docs, conv=conv_input, gate=gate_input,
        mix=mix_grad, cw=conv_weight, step_raw=step_raw, step_bias=step_bias[None],
        rate_log=rate_log[None], skip_gain=skip_gain[None], b_in=input_coeff, c_in=output_coeff,
    )
    outputs = dict(
        gq=((rows, width), BF16), gk=((rows, width), BF16), gv=((rows, width), BF16),
        gconv=((rows, channels), BF16), ggate=((rows, channels), BF16),
        gstep=((rows, ssm_heads), F32), gb=((rows, LANES), F32), gc=((rows, LANES), F32),
        gcw=((KERNEL, channels), F32), small=((PAD, LANES), F32),
    )
    scratch = dict(
        send=vm((heads, 4, rows, WIDE), BF16),
        kv=vm((per, 2, 2 * span, WIDE), BF16),
        qd=vm((per, 2, span, WIDE), BF16),
        dq=vm((per, span, WIDE), BF16),
        dkv=vm((per, 2, 2 * span, WIDE), F32),
        bks=vm((per, 2, span, WIDE), BF16),
        bkr=vm((per, 2, span, WIDE), BF16),
        kvo=vm((per, 2, span, WIDE), BF16),
        fin=vm((heads, 3, rows, WIDE), BF16),
        dcol=vm((2 * span, LANES), F32),
        mext=vm((rows + PAD, LANES), F32),
        mask=vm((KERNEL - 1, rows, LANES), F32),
        bias=vm((rows, rows), F32), pair=vm((rows, rows), F32), dpair=vm((rows, rows), F32),
        raw=vm((rows, LANES), F32), head_rows=vm((PAD, LANES), F32),
        cum=vm((rows, LANES), F32), cumt=vm((LANES, rows), F32), size=vm((rows, LANES), F32),
        enter=vm((rows, LANES), F32), to_end=vm((rows, LANES), F32),
        zsum=vm((rows, LANES), F32), usum=vm((rows, LANES), F32), acc=vm((PAD, LANES), F32),
        b=vm((rows, STATE), BF16), c=vm((rows, STATE), BF16),
        bt=vm((STATE, rows), BF16), ct=vm((STATE, rows), BF16),
        db=vm((rows, STATE), F32), dc=vm((rows, STATE), F32),
        xp=vm((rows + PAD, LANES), F32), dpad=vm((KERNEL, rows + 2 * PAD, LANES), F32),
        tail=vm((EDGE, channels), BF16), edge=vm((PAD, channels), F32),
        spill=vm((PAD, channels), F32), keep=vm((EDGE, channels), F32),
        st_s=vm((group, 2, STATE, cw), BF16), st_a=vm((group, 2, STATE, cw), BF16),
        th_s=vm((group, PAD, cw), F32), th_a=vm((group, PAD, cw), F32),
        agg=vm((2, STATE, cw), BF16), aggt=vm((PAD, cw), F32),
        up=vm((reach + 1, STATE, cw), BF16), dn=vm((reach + 1, STATE, cw), BF16),
        upt=vm((reach + 1, PAD, cw), F32), dnt=vm((reach + 1, PAD, cw), F32),
        ent_s=vm((group, 2, STATE, cw), BF16), ent=vm((group, 2, STATE, cw), BF16),
        red_s=vm((group, PAD, cw), F32), red_a=vm((group, PAD, cw), F32),
        red_p=vm((PAD, cw), F32), red_z=vm((planes, PAD, cw), F32),
        red_t=vm((PAD, cw), F32), red_o=vm((group, PAD, cw), F32),
        co_s=vm((2, rows, LANES), F32), co_a=vm((head_count, 2, rows, LANES), F32),
        one_s=dma((2,)), one_r=dma((2,)),
    )
    for name in ("kv", "qd", "fw", "bk", "dq", "do"):
        scratch[f"{name}_s"], scratch[f"{name}_r"] = dma((per, group)), dma((per, group))
    for name, size in (("st_s", group), ("th_s", group), ("co_s", head_count)):
        scratch[f"{name}s"], scratch[f"{name}r"] = dma((size,)), dma((size,))
    for name in ("up", "ut", "dn", "dt"):
        scratch[f"{name}_s"], scratch[f"{name}_r"] = dma((reach + 1,)), dma((reach + 1,))
    for name in ("en", "ra", "ro"):
        scratch[f"{name}_s"], scratch[f"{name}_r"] = dma((group,)), dma((group,))
    scratch["rz_s"], scratch["rz_r"] = dma((planes,)), dma((planes,))

    sizes = types.SimpleNamespace(
        rows=rows, channels=channels, heads=heads, ssm_heads=ssm_heads, group=group, per=per,
        chunk=chunk, chunks=chunks, padded=pairs % group != 0, count=count, reach=reach,
        head_count=head_count, names=[*inputs, *outputs, *scratch],
    )
    vmem = pl.BlockSpec(memory_space=pltpu.VMEM)
    gq, gk, gv, gconv, ggate, gstep, gb, gc, gcw, small = pl.pallas_call(
        functools.partial(kernel, sizes),
        in_specs=[vmem] * len(inputs),
        out_specs=[vmem] * len(outputs),
        out_shape=[jax.ShapeDtypeStruct(*o) for o in outputs.values()],
        scratch_shapes=list(scratch.values()),
        name="pair",
        compiler_params=pltpu.CompilerParams(
            vmem_limit_bytes=67_043_328, has_side_effects=True
        ),
        cost_estimate=pl.CostEstimate(
            flops=60_000_000_000, bytes_accessed=20_000_000, transcendentals=0
        ),
    )(*inputs.values())
    bias, rate, skip = (small[KERNEL + n, :ssm_heads] for n in range(3))
    return gq, gk, gv, gconv, ggate, gstep, gb, gc, gcw, bias, rate, skip


def solution(mesh):
    sharded = P("seq", "head")
    return jax.shard_map(
        local,
        mesh=mesh,
        in_specs=(
            sharded, sharded, sharded, sharded, P(), sharded, P(None, "head"), sharded,
            P("head"), P("head"), P("head"), P("seq", None), P("seq", None), sharded, sharded,
        ),
        out_specs=(
            sharded, sharded, sharded, sharded, sharded, sharded,
            P("seq", None), P("seq", None), P(None, "head"), P("head"), P("head"), P("head"),
        ),
        check_vma=False,
    )
```

```python
import functools
import types

import jax
import jax.numpy as jnp
from jax import lax
from jax.experimental import pallas as pl
from jax.experimental.pallas import tpu as pltpu
from jax.sharding import PartitionSpec as P

HEAD_DIM = 224
WIDE = 256
WINDOW = 1024
SSM_HEADS = 112
STATE = 64
GROUPS = 2
KERNEL = 4
PAD = 8
EDGE = 16
LANES = 128

EXACT = lax.Precision.HIGHEST
F32 = jnp.float32
BF16 = jnp.bfloat16
NEG_FILL = -1e30
SCALE = HEAD_DIM ** (-0.5)
MESH = pl.DeviceIdType.MESH


def dot(a, b, ca, cb, precision=None):
    return lax.dot_general(
        a, b, (((ca,), (cb,)), ((), ())), preferred_element_type=F32, precision=precision
    )


def aligned(first, size):
    return pl.ds(pl.multiple_of(first, size), size)


def iota(shape, dim):
    return lax.broadcasted_iota(jnp.int32, shape, dim)


class Exchange:
    def __init__(self, make, offsets):
        self.make, self.offsets = make, offsets

    def start(self):
        for d in self.offsets:
            self.make(d).start()

    def wait_recv(self):
        for d in self.offsets:
            self.make(d).wait_recv()

    def wait_send(self):
        for d in self.offsets:
            self.make(d).wait_send()


def remote(src, dst, sems, where, **device):
    return pltpu.make_async_remote_copy(
        src_ref=src, dst_ref=dst, send_sem=sems[0].at[where], recv_sem=sems[1].at[where],
        device_id=device, device_id_type=MESH,
    )


def expand(values, index):
    return jnp.take_along_axis(values, index, axis=1, mode="promise_in_bounds")


def turned(value):
    return value.astype(F32).T


def kernel(z, *refs):
    r = types.SimpleNamespace(**dict(zip(z.names, refs)))
    R, C, H, Hs, G = z.rows, z.channels, z.heads, z.ssm_heads, z.group
    per, span, CW = z.per, z.group * z.rows, z.chunk * LANES
    index = lax.axis_index("seq")
    head = lax.axis_index("head")
    place = lax.rem(index, G)
    base = index - place
    plane = lax.div(index, G)
    part = lax.div(head * Hs, SSM_HEADS // GROUPS)
    others = range(1, G)
    has_next, has_prev = index + G < z.count, index >= G

    def to_place(d):
        return lax.rem(place + d, G)

    def from_place(d):
        return lax.rem(place + G - d, G)

    def ring(at):
        return lax.rem(at + z.count, z.count)

    def kv_out(hh, d):
        p = to_place(d)
        return remote(
            r.send.at[per * p + hh, pl.ds(0, 2)], r.kv.at[hh, :, aligned(span + place * R, R)],
            (r.kv_s, r.kv_r), (hh, d), seq=base + p,
        )

    def qd_out(hh, d):
        p = to_place(d)
        return remote(
            r.send.at[per * p + hh, pl.ds(2, 2)], r.qd.at[hh, :, aligned(place * R, R)],
            (r.qd_s, r.qd_r), (hh, d), seq=base + p,
        )

    def forward(hh, d):
        p = from_place(d)
        return remote(
            r.kv.at[hh, :, aligned(span + p * R, R)], r.kv.at[hh, :, aligned(p * R, R)],
            (r.fw_s, r.fw_r), (hh, d), seq=ring(index + G),
        )

    def backward(hh, b):
        return remote(
            r.bks.at[hh, :, aligned(b * R, R)], r.bkr.at[hh, :, aligned(b * R, R)],
            (r.bk_s, r.bk_r), (hh, b), seq=ring(index - G),
        )

    def dq_out(hh, d):
        p = to_place(d)
        return remote(
            r.dq.at[hh, aligned(p * R, R)], r.fin.at[per * place + hh, 0],
            (r.dq_s, r.dq_r), (hh, d), seq=base + p,
        )

    def dkv_out(hh, d):
        p = to_place(d)
        return remote(
            r.kvo.at[hh, :, aligned(p * R, R)], r.fin.at[per * place + hh, pl.ds(1, 2)],
            (r.do_s, r.do_r), (hh, d), seq=base + p,
        )

    def tail_out():
        return remote(
            r.conv.at[pl.ds(R - EDGE, EDGE)], r.tail, (r.one_s, r.one_r), 0, seq=ring(index + 1)
        )

    def spill_out():
        return remote(r.edge, r.spill, (r.one_s, r.one_r), 1, seq=ring(index - 1))

    def state_out(d):
        p = to_place(d)
        return remote(r.st_s.at[p], r.st_a.at[place], (r.st_ss, r.st_sr), d, seq=base + p)

    def decay_out(d):
        p = to_place(d)
        return remote(r.th_s.at[p], r.th_a.at[place], (r.th_ss, r.th_sr), d, seq=base + p)

    def up_out(k):
        return remote(r.agg.at[0], r.up.at[k], (r.up_s, r.up_r), k, seq=ring(index + k * G))

    def up_decay(k):
        return remote(r.aggt, r.upt.at[k], (r.ut_s, r.ut_r), k, seq=ring(index + k * G))

    def down_out(k):
        return remote(r.agg.at[1], r.dn.at[k], (r.dn_s, r.dn_r), k, seq=ring(index - k * G))

    def down_decay(k):
        return remote(r.aggt, r.dnt.at[k], (r.dt_s, r.dt_r), k, seq=ring(index - k * G))

    def enter_out(d):
        p = to_place(d)
        return remote(r.ent_s.at[p], r.ent.at[place], (r.en_s, r.en_r), d, seq=base + p)

    def sum_out(d):
        p = to_place(d)
        return remote(r.red_s.at[p], r.red_a.at[place], (r.ra_s, r.ra_r), d, seq=base + p)

    def plane_out(k):
        return remote(
            r.red_p, r.red_z.at[plane], (r.rz_s, r.rz_r), k, seq=ring(index + k * G)
        )

    def total_out(d):
        return remote(r.red_t, r.red_o.at[place], (r.ro_s, r.ro_r), d, seq=base + to_place(d))

    def coeff_out(d):
        return remote(
            r.co_s, r.co_a.at[head], (r.co_ss, r.co_sr), d, head=lax.rem(head + d, z.head_count)
        )

    head_others = range(1, z.head_count)
    planes = z.count // G
    reach = range(1, z.reach + 1)

    @pl.when(index + 1 < z.count)
    def _():
        tail_out().start()

    @pl.when(index == 0)
    def _():
        r.tail[...] = jnp.zeros_like(r.tail)

    def window(h, ref):
        first = h * HEAD_DIM // LANES * LANES
        last = -(-(h + 1) * HEAD_DIM // LANES) * LANES
        return first, last, h * HEAD_DIM - first

    def pack(ref, h, a):
        first, last, off = window(h, ref)
        value = ref[:, first:last].astype(F32)
        if off:
            value = pltpu.roll(value, last - first - off, 1)
        value = value[:, :WIDE]
        keep = iota((R, WIDE), 1) < HEAD_DIM
        r.send[h, a] = jnp.where(keep, value, 0.0).astype(BF16)

    def own_piece(hh):
        mine = per * place + hh
        for a in range(2):
            r.kv[hh, a, aligned(span + place * R, R), :] = r.send[mine, a]
            r.qd[hh, a, aligned(place * R, R), :] = r.send[mine, 2 + a]

    def pack_all(hh):
        for a, ref in enumerate((r.k, r.v, r.q, r.do)):
            for p in range(G):
                pack(ref, per * p + hh, a)

    def send_all(hh):
        for d in others:
            kv_out(hh, d).start()
        for d in others:
            qd_out(hh, d).start()
        own_piece(hh)

        @pl.when(has_next)
        def _():
            forward(hh, 0).start()

    pack_all(0)
    send_all(0)
    for hh in range(1, per):
        pack_all(hh)

    @pl.when(jnp.logical_not(has_prev))
    def _():
        for hh in range(per):
            for a in range(2):
                r.kv[hh, a, pl.ds(0, span), :] = jnp.zeros((span, WIDE), BF16)

    @pl.when(jnp.logical_not(has_next))
    def _():
        r.bkr[...] = jnp.zeros_like(r.bkr)

    def pass_on(hh, d):
        kv_out(hh, d).wait_recv()

        @pl.when(has_next)
        def _():
            forward(hh, d).start()

    for t in range(2 * G):
        row = r.docs[pl.ds(base + t, 1), :]
        r.dcol[t * R : (t + 1) * R, :] = jnp.broadcast_to(row, (LANES, R)).T
    own_doc = span + place * R
    r.mext[...] = r.dcol[pl.ds(pl.multiple_of(own_doc - PAD, PAD), R + PAD), :]
    doc_now = r.mext[PAD:, :]
    for lag in range(1, KERNEL):
        r.mask[lag - 1] = (r.mext[PAD - lag : PAD - lag + R, :] == doc_now).astype(F32)
    i2, j2 = iota((R, R), 0), iota((R, R), 1)
    doc_row = r.docs[pl.ds(index + G, 1), :]
    doc_pair = jnp.concatenate([doc_now] * (R // LANES), axis=1)
    r.bias[...] = jnp.where((i2 >= j2) & (doc_pair == doc_row), 0.0, NEG_FILL)

    r.raw[...] = jnp.zeros_like(r.raw)
    r.raw[:, :Hs] = r.step_raw[...] + r.step_bias[...]
    r.head_rows[...] = jnp.zeros_like(r.head_rows)
    r.head_rows[0:1, :Hs] = jnp.exp(r.rate_log[...])
    r.head_rows[1:2, :Hs] = r.skip_gain[...]
    raw = r.raw[...]
    rate = r.head_rows[0:1, :]
    size_all = jnp.maximum(raw, 0.0) + jnp.log1p(jnp.exp(-jnp.abs(raw)))
    log_decay = -size_all * rate
    tri = (i2 >= j2).astype(F32)
    cum = dot(tri, log_decay, 1, 0, EXACT)
    enter_all = jnp.where(doc_now == r.mext[PAD - 1 : PAD, :], jnp.exp(cum), 0.0)
    to_end_all = jnp.where(
        doc_now == r.mext[R + PAD - 1 : R + PAD, :], jnp.exp(cum[R - 1 : R, :] - cum), 0.0
    )
    r.cum[...] = cum
    r.cumt[...] = cum.T
    r.size[...] = size_all
    r.enter[...] = enter_all
    r.to_end[...] = to_end_all

    b_wide, c_wide = r.b_in[...], r.c_in[...]
    b_own, c_own = b_wide[:, :STATE], c_wide[:, :STATE]
    for g in range(1, GROUPS):
        b_own = jnp.where(part == g, b_wide[:, g * STATE : (g + 1) * STATE], b_own)
        c_own = jnp.where(part == g, c_wide[:, g * STATE : (g + 1) * STATE], c_own)
    r.b[...] = b_own
    r.c[...] = c_own
    r.bt[...] = turned(b_own).astype(BF16)
    r.ct[...] = turned(c_own).astype(BF16)
    r.pair[...] = dot(c_own, b_own, 1, 1)

    @pl.when(index > 0)
    def _():
        tail_out().wait_recv()

    lower = iota((R, LANES), 1) < LANES // 2
    half = jnp.where(lower, 0, 1)

    def conv_pre(lanes):
        r.xp[:PAD, :] = r.tail[:, lanes].astype(F32)[EDGE - PAD :, :]
        r.xp[PAD:, :] = r.conv[:, lanes].astype(F32)
        pre = r.cw[0:1, lanes] * r.xp[PAD:, :]
        for lag in range(1, KERNEL):
            pre = pre + r.cw[lag : lag + 1, lanes] * (
                r.xp[PAD - lag : PAD - lag + R, :] * r.mask[lag - 1]
            )
        return pre

    def ends(c):
        def one(m, carry):
            p = c * z.chunk + m
            lanes = aligned(p * LANES, LANES)
            here = aligned(m * LANES, LANES)
            pre = conv_pre(lanes)
            act = pre * jax.nn.sigmoid(pre)
            who = half + 2 * p
            enter = expand(r.enter[...], who)
            weighted = act * expand(r.size[...], who) * expand(r.to_end[...], who)
            r.st_s[c, 0, :, here] = dot(r.bt[...], weighted.astype(BF16), 1, 0).astype(BF16)
            gate = r.gate[:, lanes].astype(F32)
            dy = r.mix[:, lanes].astype(F32) * (gate * jax.nn.sigmoid(gate))
            r.st_s[c, 1, :, here] = dot(r.ct[...], (dy * enter).astype(BF16), 1, 0).astype(BF16)
            r.th_s[c, :, here] = jnp.broadcast_to(enter[R - 1 : R, :], (PAD, LANES))
            return carry

        lax.fori_loop(0, z.chunks[c], one, 0)

    if z.padded:
        r.st_s[...] = jnp.zeros_like(r.st_s)
        r.th_s[...] = jnp.zeros_like(r.th_s)
        r.red_s[...] = jnp.zeros_like(r.red_s)

    for c in range(G):
        ends(c)
        if c > 0:
            pass_on(0, c)
    state, decay = Exchange(state_out, others), Exchange(decay_out, others)
    decay.start()
    state.start()
    for hh in range(1, per):
        send_all(hh)
    r.st_a[place] = r.st_s[place]
    r.th_a[place] = r.th_s[place]

    r.dkv[...] = jnp.zeros_like(r.dkv)

    def attention(hh):
        j, i = iota((R, R), 0), iota((R, R), 1)

        def block(b, carry):
            mine = aligned(b * R, R)
            q = r.qd[hh, 0, mine, :]
            grad = r.qd[hh, 1, mine, :]
            docq = r.docs[pl.ds(base + G + b, 1), :]
            places = [aligned((b + G - gap) * R, R) for gap in range(G + 1)]
            scores = []
            top = None
            for gap in range(G + 1):
                dock = r.dcol[places[gap], :]
                allowed = jnp.concatenate([dock] * (R // LANES), axis=1) == docq
                if gap == 0:
                    allowed = allowed & (i >= j)
                if gap == G:
                    allowed = allowed & (i < j)
                s = jnp.where(allowed, dot(r.kv[hh, 0, places[gap], :], q, 1, 1) * SCALE, NEG_FILL)
                scores.append(s)
                m = jnp.max(s, axis=0, keepdims=True)
                top = m if top is None else jnp.maximum(top, m)
            total = None
            expo = []
            for gap in range(G + 1):
                e = jnp.exp(scores[gap] - top)
                expo.append(e)
                t = jnp.sum(e, axis=0, keepdims=True)
                total = t if total is None else total + t
            inverse = 1.0 / jnp.maximum(total, 1.0)
            delta = None
            dprobs = []
            for gap in range(G + 1):
                weight = (expo[gap] * inverse).astype(BF16)
                dp = dot(r.kv[hh, 1, places[gap], :], grad, 1, 1)
                d = jnp.sum(weight.astype(F32) * dp, axis=0, keepdims=True)
                delta = d if delta is None else delta + d
                r.dkv[hh, 1, places[gap], :] += dot(weight, grad, 1, 0)
                dprobs.append(dp)
            dq = None
            for gap in range(G + 1):
                ds = (expo[gap] * inverse * (dprobs[gap] - delta)).astype(BF16)
                r.dkv[hh, 0, places[gap], :] += dot(ds, q, 1, 0)
                piece = dot(ds, r.kv[hh, 0, places[gap], :], 0, 0)
                dq = piece if dq is None else dq + piece
            r.dq[hh, mine, :] = (dq * SCALE).astype(BF16)

            @pl.when(has_prev)
            def _():
                for a in range(2):
                    r.bks[hh, a, mine, :] = r.dkv[hh, a, mine, :].astype(BF16)
                backward(hh, b).start()

            return carry

        lax.fori_loop(0, G, block, 0)
        for d in others:
            dq_out(hh, d).start()
        r.fin[per * place + hh, 0] = r.dq[hh, aligned(place * R, R), :]

    def attention_inputs(hh):
        for d in others:
            qd_out(hh, d).wait_recv()

        @pl.when(has_prev)
        def _():
            for d in range(G):
                forward(hh, d).wait_recv()

    def give_back(hh):
        @pl.when(has_next)
        def _():
            for b in range(G):
                backward(hh, b).wait_recv()

        for t in range(G):
            rows = slice(t * R, (t + 1) * R)
            own = slice(span + t * R, span + (t + 1) * R)
            dk = (r.dkv[hh, 0, own, :] + r.bkr[hh, 0, rows, :].astype(F32)) * SCALE
            dv = r.dkv[hh, 1, own, :] + r.bkr[hh, 1, rows, :].astype(F32)
            r.kvo[hh, 0, rows, :] = dk.astype(BF16)
            r.kvo[hh, 1, rows, :] = dv.astype(BF16)
        for d in others:
            dkv_out(hh, d).start()
        for a in range(2):
            r.fin[per * place + hh, 1 + a] = r.kvo[hh, a, aligned(place * R, R), :]

    def tall(rows):
        return jnp.concatenate([rows] * (STATE // PAD), axis=0)

    def through(t, here):
        return tall(r.th_a[t, :, here])

    def chain_out():
        state.wait_recv()
        decay.wait_recv()
        def one(m, carry):
            here = aligned(m * LANES, LANES)
            a = r.st_a[0, 0, :, here].astype(F32)
            thr = r.th_a[0, :, here]
            for t in range(1, G):
                a = a * through(t, here) + r.st_a[t, 0, :, here].astype(F32)
                thr = thr * r.th_a[t, :, here]
            b = r.st_a[G - 1, 1, :, here].astype(F32)
            for t in range(G - 2, -1, -1):
                b = b * through(t, here) + r.st_a[t, 1, :, here].astype(F32)
            r.agg[0, :, here] = a.astype(BF16)
            r.agg[1, :, here] = b.astype(BF16)
            r.aggt[:, here] = thr
            return carry

        lax.fori_loop(0, z.chunk, one, 0)
        for k in reach:
            @pl.when(index + k * G < z.count)
            def _():
                up_out(k).start()
                up_decay(k).start()

            @pl.when(index + k * G >= z.count)
            def _():
                r.dn[k] = jnp.zeros((STATE, CW), BF16)
                r.dnt[k] = jnp.zeros((PAD, CW), F32)

            @pl.when(index - k * G >= 0)
            def _():
                down_out(k).start()
                down_decay(k).start()

            @pl.when(index - k * G < 0)
            def _():
                r.up[k] = jnp.zeros((STATE, CW), BF16)
                r.upt[k] = jnp.zeros((PAD, CW), F32)

    def chain_in():
        for k in reach:
            @pl.when(index - k * G >= 0)
            def _():
                up_out(k).wait_recv()
                up_decay(k).wait_recv()

            @pl.when(index + k * G < z.count)
            def _():
                down_out(k).wait_recv()
                down_decay(k).wait_recv()

        def one(m, carry):
            here = aligned(m * LANES, LANES)
            s = jnp.zeros((STATE, LANES), F32)
            e = jnp.zeros((STATE, LANES), F32)
            for k in reversed(reach):
                s = s * tall(r.upt[k, :, here]) + r.up[k, :, here].astype(F32)
                e = e * tall(r.dnt[k, :, here]) + r.dn[k, :, here].astype(F32)
            for t in range(G):
                r.ent_s[t, 0, :, here] = s.astype(BF16)
                s = s * through(t, here) + r.st_a[t, 0, :, here].astype(F32)
            for t in range(G - 1, -1, -1):
                r.ent_s[t, 1, :, here] = e.astype(BF16)
                e = e * through(t, here) + r.st_a[t, 1, :, here].astype(F32)
            return carry

        lax.fori_loop(0, z.chunk, one, 0)
        for d in others:
            enter_out(d).start()
        r.ent[place] = r.ent_s[place]

    r.dpair[...] = jnp.zeros_like(r.dpair)
    r.db[...] = jnp.zeros_like(r.db)
    r.dc[...] = jnp.zeros_like(r.dc)
    r.zsum[...] = jnp.zeros_like(r.zsum)
    r.usum[...] = jnp.zeros_like(r.usum)
    r.acc[...] = jnp.zeros_like(r.acc)
    r.dpad[...] = jnp.zeros_like(r.dpad)
    lane = iota((R, LANES), 1)
    lane_row = iota((PAD, LANES), 1)

    def mixer(c):
        def one(m, carry):
            p = c * z.chunk + m
            lanes = aligned(p * LANES, LANES)
            here = aligned(m * LANES, LANES)
            who = half + 2 * p
            size = expand(r.size[...], who)
            enter = expand(r.enter[...], who)
            to_end = expand(r.to_end[...], who)
            pre = conv_pre(lanes)
            sig_pre = jax.nn.sigmoid(pre)
            act = pre * sig_pre
            x_half = (act * size).astype(BF16)
            gate = r.gate[:, lanes].astype(F32)
            sig_gate = jax.nn.sigmoid(gate)
            silu_gate = gate * sig_gate
            cot = r.mix[:, lanes].astype(F32)
            dy = cot * silu_gate
            dy_half = dy.astype(BF16)
            state_in = r.ent[c, 0, :, here]
            end_cot = r.ent[c, 1, :, here]
            zero = jnp.zeros_like(dy_half)
            y_parts, dx_parts = [], []
            dpair = r.dpair[...]
            for k in range(2):
                column = expand(r.cum[...], jnp.zeros((R, LANES), jnp.int32) + (2 * p + k))
                column = jnp.concatenate([column] * (R // LANES), axis=1)
                weights = jnp.exp((column - r.cumt[pl.ds(2 * p + k, 1), :]) + r.bias[...])
                mixing = (r.pair[...] * weights).astype(BF16)
                y_parts.append(dot(mixing, x_half, 1, 0))
                dx_parts.append(dot(mixing, dy_half, 0, 0))
                dy_one = jnp.where(lower if k == 0 else ~lower, dy_half, zero)
                dpair = dpair + dot(dy_one, x_half, 1, 1) * weights
            r.dpair[...] = dpair
            inner = jnp.where(lower, y_parts[0], y_parts[1]) + enter * dot(r.c[...], state_in, 1, 0)
            end_part = to_end * dot(r.b[...], end_cot, 1, 0)
            dx = jnp.where(lower, dx_parts[0], dx_parts[1]) + end_part
            skip = expand(jnp.broadcast_to(r.head_rows[1:2, :], (PAD, LANES)), who[:PAD])[0:1]
            y = inner + skip * act
            r.ggate[:, lanes] = (cot * y * (sig_gate + silu_gate * (1.0 - sig_gate))).astype(BF16)
            x_wide = x_half.astype(F32)
            zed = dy_half.astype(F32) * inner - x_wide * dx
            you = dx * act
            r.dc[...] += dot((enter * dy).astype(BF16), state_in, 1, 1)
            r.db[...] += dot((to_end * x_wide).astype(BF16), end_cot, 1, 1)
            dact = dx * size + skip * dy
            dpre = dact * (sig_pre + act * (1.0 - sig_pre))
            sums = [jnp.sum(dpre * r.xp[PAD:, :], axis=0, keepdims=True)]
            r.dpad[0, PAD : PAD + R, :] = dpre
            grown = r.cw[0:1, lanes] * r.dpad[0, 0 : R + PAD, :]
            for lag in range(1, KERNEL):
                masked = dpre * r.mask[lag - 1]
                sums.append(
                    jnp.sum(masked * r.xp[PAD - lag : PAD - lag + R, :], axis=0, keepdims=True)
                )
                r.dpad[lag, PAD : PAD + R, :] = masked
                grown = grown + r.cw[lag : lag + 1, lanes] * r.dpad[lag, lag : lag + R + PAD, :]
            r.gconv[:, lanes] = grown[PAD:, :].astype(BF16)
            r.edge[:, lanes] = grown[:PAD, :]
            r.keep[:, lanes] = grown[R + PAD - EDGE :, :]
            none = jnp.zeros((PAD - KERNEL, LANES), F32)
            r.red_s[c, :, here] = jnp.concatenate(sums + [none], axis=0)
            heads3 = jnp.concatenate(
                [
                    jnp.sum(dy * act, axis=0, keepdims=True),
                    jnp.sum(state_in.astype(F32) * end_cot.astype(F32), axis=0, keepdims=True),
                    jnp.sum(x_wide * end_part, axis=0, keepdims=True),
                    jnp.zeros((PAD - 3, LANES), F32),
                ],
                axis=0,
            )
            for k in range(2):
                side = lower if k == 0 else ~lower
                mine = lane == 2 * p + k
                z_one = jnp.sum(jnp.where(side, zed, 0.0), axis=1, keepdims=True)
                u_one = jnp.sum(jnp.where(side, you, 0.0), axis=1, keepdims=True)
                h_one = jnp.sum(jnp.where(side[:PAD], heads3, 0.0), axis=1, keepdims=True)
                r.zsum[...] = jnp.where(mine, z_one, r.zsum[...])
                r.usum[...] = jnp.where(mine, u_one, r.usum[...])
                r.acc[...] = jnp.where(lane_row == 2 * p + k, h_one, r.acc[...])
            return carry

        lax.fori_loop(0, z.chunks[c], one, 0)

    def mixer_start():
        for d in others:
            enter_out(d).wait_recv()

    def mixer_end():
        @pl.when(index > 0)
        def _():
            spill_out().start()

        total = r.dpair[...]
        dc = r.dc[...] + dot(total, r.b[...].astype(F32), 1, 0, EXACT)
        db = r.db[...] + dot(total, r.c[...].astype(F32), 0, 0, EXACT)
        mine = lax.div(lane, STATE) == part
        r.co_s[0] = jnp.where(mine, jnp.concatenate([db] * GROUPS, axis=1), 0.0)
        r.co_s[1] = jnp.where(mine, jnp.concatenate([dc] * GROUPS, axis=1), 0.0)
        for d in head_others:
            coeff_out(d).start()
        r.co_a[head] = r.co_s[...]
        last_row = r.acc[2:3, :] + r.enter[R - 1 : R, :] * r.acc[1:2, :]
        rows = iota((R, LANES), 0)
        dcum = r.zsum[...] + jnp.where(rows == R - 1, last_row, 0.0)
        upper = (iota((R, R), 0) <= iota((R, R), 1)).astype(F32)
        dlog = dot(upper, dcum, 1, 0, EXACT)
        rates = r.head_rows[0:1, :]
        grad_step = (r.usum[...] - dlog * rates) * jax.nn.sigmoid(r.raw[...])
        r.gstep[...] = grad_step[:, :Hs]
        small = jnp.concatenate(
            [
                jnp.zeros((KERNEL, LANES), F32),
                jnp.sum(grad_step, axis=0, keepdims=True),
                jnp.sum(dlog * (-r.size[...] * rates), axis=0, keepdims=True),
                r.acc[0:1, :],
                jnp.zeros((1, LANES), F32),
            ],
            axis=0,
        )
        r.red_s[0, :, 0:LANES] += small
        for d in others:
            sum_out(d).start()
        r.red_a[place] = r.red_s[place]

    def sums_planes():
        for d in others:
            sum_out(d).wait_recv()
        total = r.red_a[0]
        for t in range(1, G):
            total = total + r.red_a[t]
        r.red_p[...] = total
        for k in range(1, planes):
            plane_out(k).start()
        r.red_z[plane] = total

    def sums_all():
        for k in range(1, planes):
            plane_out(k).wait_recv()
        total = r.red_z[0]
        for t in range(1, planes):
            total = total + r.red_z[t]
        r.red_t[...] = total
        for d in others:
            total_out(d).start()
        r.red_o[place] = total

    def sums_end():
        for d in others:
            total_out(d).wait_recv()
        for c in range(G):
            width = z.chunks[c] * LANES
            if width:
                r.gcw[:, c * CW : c * CW + width] = r.red_o[c, 0:KERNEL, 0:width]
        r.small[...] = r.red_o[0, :, 0:LANES]
        for d in head_others:
            coeff_out(d).wait_recv()
        db, dc = r.co_a[0, 0], r.co_a[0, 1]
        for d in head_others:
            db = db + r.co_a[d, 0]
            dc = dc + r.co_a[d, 1]
        r.gb[...] = db
        r.gc[...] = dc

        @pl.when(index + 1 < z.count)
        def _():
            spill_out().wait_recv()

        @pl.when(index + 1 >= z.count)
        def _():
            r.spill[...] = jnp.zeros_like(r.spill)

        spill = jnp.concatenate([jnp.zeros((EDGE - PAD, C), F32), r.spill[...]], axis=0)
        r.gconv[R - EDGE :, :] = (r.keep[...] + spill).astype(BF16)

    def unpack(arrays, arriving):
        for hh in range(per):
            for d in others:
                arriving(hh, d).wait_recv()
        for a, ref in arrays:
            open_tile = None
            for h in range(H):
                first, last, off = window(h, ref)
                value = r.fin[h, a].astype(F32)
                if last - first > WIDE:
                    value = jnp.concatenate([value, jnp.zeros((R, LANES), F32)], axis=1)
                if off:
                    value = pltpu.roll(value, off, 1)
                tiles = [value[:, n : n + LANES] for n in range(0, last - first, LANES)]
                if off:
                    tiles[0] = tiles[0] + open_tile
                done = (h + 1) * HEAD_DIM % LANES == 0
                for n, tile in enumerate(tiles if done else tiles[:-1]):
                    ref[:, first + n * LANES : first + (n + 1) * LANES] = tile.astype(BF16)
                open_tile = tiles[-1]

    attention_inputs(0)
    attention(0)
    chain_out()
    for hh in range(1, per):
        for d in others:
            pass_on(hh, d)
    chain_in()
    for hh in range(1, per):
        attention_inputs(hh)
        attention(hh)
    for hh in range(per - 1):
        give_back(hh)
    mixer_start()
    for c in range(G):
        if c == G - 1:
            unpack(((0, r.gq),), dq_out)
            give_back(per - 1)
        mixer(c)
    mixer_end()
    sums_planes()
    sums_all()
    unpack(((1, r.gk), (2, r.gv)), dkv_out)
    sums_end()

    for hh in range(per):
        for d in others:
            kv_out(hh, d).wait_send()
            qd_out(hh, d).wait_send()
            dq_out(hh, d).wait_send()
            dkv_out(hh, d).wait_send()

    @pl.when(has_next)
    def _():
        for hh in range(per):
            for d in range(G):
                forward(hh, d).wait_send()

    @pl.when(has_prev)
    def _():
        for hh in range(per):
            for b in range(G):
                backward(hh, b).wait_send()

    state.wait_send()
    decay.wait_send()
    for d in others:
        enter_out(d).wait_send()
        sum_out(d).wait_send()
        total_out(d).wait_send()
    for k in range(1, planes):
        plane_out(k).wait_send()
    for d in head_others:
        coeff_out(d).wait_send()
    for k in reach:
        @pl.when(index + k * G < z.count)
        def _():
            up_out(k).wait_send()
            up_decay(k).wait_send()

        @pl.when(index - k * G >= 0)
        def _():
            down_out(k).wait_send()
            down_decay(k).wait_send()

    @pl.when(index + 1 < z.count)
    def _():
        tail_out().wait_send()

    @pl.when(index > 0)
    def _():
        spill_out().wait_send()


def copy_kernel(*refs):
    for source, target in zip(refs[: len(refs) // 2], refs[len(refs) // 2 :]):
        target[...] = source[...]


def written(arrays, steps=7):
    large = lambda a: a.shape[1] % (steps * LANES) == 0 and a.dtype == BF16
    spec = lambda a: (
        pl.BlockSpec((a.shape[0], a.shape[1] // steps), lambda n: (0, n))
        if large(a) else pl.BlockSpec(a.shape, lambda n: (0, 0))
    )
    specs = [spec(a) for a in arrays]
    return pl.pallas_call(
        copy_kernel,
        grid=(steps,),
        in_specs=specs,
        out_specs=specs,
        out_shape=[jax.ShapeDtypeStruct(a.shape, a.dtype) for a in arrays],
        name="written",
        compiler_params=pltpu.CompilerParams(
            dimension_semantics=("arbitrary",), vmem_limit_bytes=67_043_328
        ),
        cost_estimate=pl.CostEstimate(
            flops=2_000_000_000, bytes_accessed=14_000_000, transcendentals=0
        ),
    )(*arrays)


def local(
    queries, keys, values, attn_grad, doc_ids, conv_input, conv_weight, step_raw, step_bias,
    rate_log, skip_gain, input_coeff, output_coeff, gate_input, mix_grad,
):
    rows, width = queries.shape
    channels = conv_input.shape[1]
    ssm_heads = step_raw.shape[1]
    heads = width // HEAD_DIM
    count, head_count = lax.axis_size("seq"), lax.axis_size("head")
    group = WINDOW // rows
    pairs = channels // LANES
    chunk = -(-pairs // group)
    chunks = [max(0, min(chunk, pairs - c * chunk)) for c in range(group)]
    per = heads // group
    span, cw, planes = group * rows, chunk * LANES, count // group
    reach = max(1, min(planes - 1, -(-(count // 2) // group)))
    docs = jnp.pad(doc_ids.astype(F32), (span, 0), constant_values=-1.0).reshape(count + group, rows)

    vm, dma = pltpu.VMEM, pltpu.SemaphoreType.DMA
    inputs = dict(
        q=queries, k=keys, v=values, do=attn_grad, docs=docs, conv=conv_input, gate=gate_input,
        mix=mix_grad, cw=conv_weight, step_raw=step_raw, step_bias=step_bias[None],
        rate_log=rate_log[None], skip_gain=skip_gain[None], b_in=input_coeff, c_in=output_coeff,
    )
    outputs = dict(
        gq=((rows, width), BF16), gk=((rows, width), BF16), gv=((rows, width), BF16),
        gconv=((rows, channels), BF16), ggate=((rows, channels), BF16),
        gstep=((rows, ssm_heads), F32), gb=((rows, LANES), F32), gc=((rows, LANES), F32),
        gcw=((KERNEL, channels), F32), small=((PAD, LANES), F32),
    )
    scratch = dict(
        send=vm((heads, 4, rows, WIDE), BF16),
        kv=vm((per, 2, 2 * span, WIDE), BF16),
        qd=vm((per, 2, span, WIDE), BF16),
        dq=vm((per, span, WIDE), BF16),
        dkv=vm((per, 2, 2 * span, WIDE), F32),
        bks=vm((per, 2, span, WIDE), BF16),
        bkr=vm((per, 2, span, WIDE), BF16),
        kvo=vm((per, 2, span, WIDE), BF16),
        fin=vm((heads, 3, rows, WIDE), BF16),
        dcol=vm((2 * span, LANES), F32),
        mext=vm((rows + PAD, LANES), F32),
        mask=vm((KERNEL - 1, rows, LANES), F32),
        bias=vm((rows, rows), F32), pair=vm((rows, rows), F32), dpair=vm((rows, rows), F32),
        raw=vm((rows, LANES), F32), head_rows=vm((PAD, LANES), F32),
        cum=vm((rows, LANES), F32), cumt=vm((LANES, rows), F32), size=vm((rows, LANES), F32),
        enter=vm((rows, LANES), F32), to_end=vm((rows, LANES), F32),
        zsum=vm((rows, LANES), F32), usum=vm((rows, LANES), F32), acc=vm((PAD, LANES), F32),
        b=vm((rows, STATE), BF16), c=vm((rows, STATE), BF16),
        bt=vm((STATE, rows), BF16), ct=vm((STATE, rows), BF16),
        db=vm((rows, STATE), F32), dc=vm((rows, STATE), F32),
        xp=vm((rows + PAD, LANES), F32), dpad=vm((KERNEL, rows + 2 * PAD, LANES), F32),
        tail=vm((EDGE, channels), BF16), edge=vm((PAD, channels), F32),
        spill=vm((PAD, channels), F32), keep=vm((EDGE, channels), F32),
        st_s=vm((group, 2, STATE, cw), BF16), st_a=vm((group, 2, STATE, cw), BF16),
        th_s=vm((group, PAD, cw), F32), th_a=vm((group, PAD, cw), F32),
        agg=vm((2, STATE, cw), BF16), aggt=vm((PAD, cw), F32),
        up=vm((reach + 1, STATE, cw), BF16), dn=vm((reach + 1, STATE, cw), BF16),
        upt=vm((reach + 1, PAD, cw), F32), dnt=vm((reach + 1, PAD, cw), F32),
        ent_s=vm((group, 2, STATE, cw), BF16), ent=vm((group, 2, STATE, cw), BF16),
        red_s=vm((group, PAD, cw), F32), red_a=vm((group, PAD, cw), F32),
        red_p=vm((PAD, cw), F32), red_z=vm((planes, PAD, cw), F32),
        red_t=vm((PAD, cw), F32), red_o=vm((group, PAD, cw), F32),
        co_s=vm((2, rows, LANES), F32), co_a=vm((head_count, 2, rows, LANES), F32),
        one_s=dma((2,)), one_r=dma((2,)),
    )
    for name in ("kv", "qd", "fw", "bk", "dq", "do"):
        scratch[f"{name}_s"], scratch[f"{name}_r"] = dma((per, group)), dma((per, group))
    for name, size in (("st_s", group), ("th_s", group), ("co_s", head_count)):
        scratch[f"{name}s"], scratch[f"{name}r"] = dma((size,)), dma((size,))
    for name in ("up", "ut", "dn", "dt"):
        scratch[f"{name}_s"], scratch[f"{name}_r"] = dma((reach + 1,)), dma((reach + 1,))
    for name in ("en", "ra", "ro"):
        scratch[f"{name}_s"], scratch[f"{name}_r"] = dma((group,)), dma((group,))
    scratch["rz_s"], scratch["rz_r"] = dma((planes,)), dma((planes,))

    sizes = types.SimpleNamespace(
        rows=rows, channels=channels, heads=heads, ssm_heads=ssm_heads, group=group, per=per,
        chunk=chunk, chunks=chunks, padded=pairs % group != 0, count=count, reach=reach,
        head_count=head_count, names=[*inputs, *outputs, *scratch],
    )
    vmem = pl.BlockSpec(memory_space=pltpu.VMEM)
    found = pl.pallas_call(
        functools.partial(kernel, sizes),
        in_specs=[vmem] * len(inputs),
        out_specs=[vmem] * len(outputs),
        out_shape=[jax.ShapeDtypeStruct(*o) for o in outputs.values()],
        scratch_shapes=list(scratch.values()),
        name="pair",
        compiler_params=pltpu.CompilerParams(
            vmem_limit_bytes=67_043_328, has_side_effects=True
        ),
        cost_estimate=pl.CostEstimate(
            flops=60_000_000_000, bytes_accessed=20_000_000, transcendentals=0
        ),
    )(*inputs.values())
    gq, gk, gv, gconv, ggate, gstep, gb, gc, gcw, small = written(found)
    bias, rate, skip = (small[KERNEL + n, :ssm_heads] for n in range(3))
    return gq, gk, gv, gconv, ggate, gstep, gb, gc, gcw, bias, rate, skip


def solution(mesh):
    sharded = P("seq", "head")
    return jax.shard_map(
        local,
        mesh=mesh,
        in_specs=(
            sharded, sharded, sharded, sharded, P(), sharded, P(None, "head"), sharded,
            P("head"), P("head"), P("head"), P("seq", None), P("seq", None), sharded, sharded,
        ),
        out_specs=(
            sharded, sharded, sharded, sharded, sharded, sharded,
            P("seq", None), P("seq", None), P(None, "head"), P("head"), P("head"), P("head"),
        ),
        check_vma=False,
    )
```
